256 devices in a mesh: dp: 32 (over z, y), vp: 8 (over x, core).
Axes of the slice: x: 4, y: 4, z: 8, core: 2. Of those that a mesh axis runs over, the one named last changes fastest.
Arguments:
- hidden: bfloat16 [96, 128, 896], P('dp')
- norm_gain: float32 [896], replicated
- emb_table: bfloat16 [151936, 896], P('vp')
- labels: int32 [96, 128], P('dp')
- tok_mask: float32 [96, 128], P('dp')
Outputs:
- output 1: float32 [], replicated
- output 2: float32 [151936, 896], P('vp')
- output 3: bfloat16 [96, 128, 896], P('dp')
- output 4: float32 [896], replicated
All inputs are finite; a program needn't handle non-finite values.
Results may differ from the reference program's by a relative error of at most 0.001.
Values sent between devices are 32-bit elements.
A program may use at most 768 MiB of HBM per device.

```python
import math
import jax
import jax.numpy as jnp
from jax import lax

WIDTH = 896
VOCAB = 151936
BATCH = 96
SEQ_LEN = 128
LOGIT_SCALE = 0.0625
EPS = 1e-5
EMB_GAIN = 48.0
TARGET_PULL = 4.0
BLOCK_ROWS = math.gcd(BATCH, max(1, 2**25 // (SEQ_LEN * VOCAB)))
NUM_BLOCKS = BATCH // BLOCK_ROWS
BLOCK_TOKENS = BLOCK_ROWS * SEQ_LEN


def setup_inputs(seed: int = 0) -> dict:
    key = jax.random.key(seed)
    key_table, key_noise, key_gain, key_labels, key_lengths = jax.random.split(key, 5)
    emb_std = EMB_GAIN / math.sqrt(WIDTH)
    emb_table = (jax.random.normal(key_table, (VOCAB, WIDTH), jnp.float32) * emb_std).astype(jnp.bfloat16)
    labels = jax.random.randint(key_labels, (BATCH, SEQ_LEN), 0, VOCAB, dtype=jnp.int32)
    target_rows = jnp.take(emb_table, labels, axis=0).astype(jnp.float32) / emb_std
    noise = jax.random.normal(key_noise, (BATCH, SEQ_LEN, WIDTH), jnp.float32)
    hidden = (noise + (TARGET_PULL / math.sqrt(WIDTH)) * target_rows).astype(jnp.bfloat16)
    lengths = jax.random.randint(key_lengths, (BATCH, 1), max(1, SEQ_LEN // 4), SEQ_LEN + 1, dtype=jnp.int32)
    tok_mask = (jnp.arange(SEQ_LEN)[None, :] < lengths).astype(jnp.float32)
    norm_gain = 1.0 + 0.25 * jax.random.normal(key_gain, (WIDTH,), jnp.float32)
    return {'hidden': hidden, 'norm_gain': norm_gain, 'emb_table': emb_table, 'labels': labels, 'tok_mask': tok_mask}


def norm_forward(tokens, norm_gain):
    values = tokens.astype(jnp.float32)
    mean_x = jnp.mean(values, axis=-1, keepdims=True)
    centered = values - mean_x
    variance = jnp.mean(centered * centered, axis=-1, keepdims=True)
    inv_std = lax.rsqrt(variance + EPS)
    x_hat = centered * inv_std
    return (norm_gain * x_hat).astype(jnp.bfloat16), x_hat, inv_std


def reference(hidden, norm_gain, emb_table, labels, tok_mask):
    count = jnp.sum(tok_mask)
    vocab_ids = jnp.arange(VOCAB)

    def block_step(carry, block):
        table_grad, gain_grad, loss_sum = carry
        tokens, block_labels, block_mask = block
        normed, x_hat, inv_std = norm_forward(tokens, norm_gain)
        logits = LOGIT_SCALE * jnp.dot(normed, emb_table.T, preferred_element_type=jnp.float32)
        log_norm = jax.nn.logsumexp(logits, axis=-1)
        hits = vocab_ids[None, :] == block_labels[:, None]
        label_logit = jnp.sum(jnp.where(hits, logits, 0.0), axis=-1)
        loss_sum = loss_sum + jnp.sum(block_mask * (log_norm - label_logit))
        soft_probs = jnp.exp(logits - log_norm[:, None])
        weight = block_mask * (LOGIT_SCALE / count)
        d_logits = (jnp.where(hits, soft_probs - 1.0, soft_probs) * weight[:, None]).astype(jnp.bfloat16)
        d_normed = jnp.dot(d_logits, emb_table, preferred_element_type=jnp.float32)
        table_grad = table_grad + jnp.dot(d_logits.T, normed, preferred_element_type=jnp.float32)
        gain_grad = gain_grad + jnp.sum(d_normed * x_hat, axis=0)
        d_xhat = d_normed * norm_gain
        mean_one = jnp.mean(d_xhat, axis=-1, keepdims=True)
        mean_two = jnp.mean(d_xhat * x_hat, axis=-1, keepdims=True)
        d_tokens = inv_std * (d_xhat - mean_one - x_hat * mean_two)
        return (table_grad, gain_grad, loss_sum), d_tokens.astype(jnp.bfloat16)

    blocks = (hidden.reshape(NUM_BLOCKS, BLOCK_TOKENS, WIDTH), labels.reshape(NUM_BLOCKS, BLOCK_TOKENS), tok_mask.reshape(NUM_BLOCKS, BLOCK_TOKENS))
    start = (jnp.zeros((VOCAB, WIDTH), jnp.float32), jnp.zeros((WIDTH,), jnp.float32), jnp.zeros((), jnp.float32))
    (table_grad, gain_grad, loss_sum), d_tokens = lax.scan(block_step, start, blocks)
    return loss_sum / count, table_grad, d_tokens.reshape(BATCH, SEQ_LEN, WIDTH), gain_grad
```

```python
import functools
import heapq

import jax
import jax.numpy as jnp
from jax import lax
from jax.experimental import pallas as pl
from jax.experimental.pallas import tpu as pltpu
from jax.sharding import PartitionSpec as P

MESH = pl.DeviceIdType.MESH
LOGIT_SCALE = 0.0625
EPS = 1e-5
NZ, NY, NV = 8, 4, 8
NDP = NZ * NY
TOK = 384
WIDTH = 896
VLOC = 18992
NALL = NDP * TOK
SPLIT = 160
COLOR_ROWS = 2304
CHUNK = 192
HALF = CHUNK // 2
NCHUNK = COLOR_ROWS // CHUNK
B_BASE = 4 * COLOR_ROWS
REST_BASE = 8 * COLOR_ROWS
REST_PARTS = ((REST_BASE, 288), (REST_BASE + 288, VLOC - REST_BASE - 288))
SLOTS = 3
TT = 2048
NT = NALL // TT
VT = 1200
NVT = -(-VLOC // VT)
SLICE = TOK // NV
F32 = jnp.float32
BF16 = jnp.bfloat16
VMEM_LIMIT = 63 * 2**20


def dot_nt(a, b):
    return lax.dot_general(a, b, (((1,), (1,)), ((), ())), preferred_element_type=F32)


def rsqrt_norm(values):
    mean_x = jnp.mean(values, axis=-1, keepdims=True)
    centered = values - mean_x
    variance = jnp.mean(centered * centered, axis=-1, keepdims=True)
    inv_std = lax.rsqrt(variance + EPS)
    return centered * inv_std, inv_std


def row_start(i):
    return pl.multiple_of(jnp.minimum(i * VT, VLOC - VT), 16)


def stats_kernel(vp_ref, hid_ref, gain_ref, lab_ref, mask_ref, emb_ref, nf_ref, st_ref, nb, m_s, s_s, l_s):
    i = pl.program_id(0)

    @pl.when(i == 0)
    def _():
        x_hat, _ = rsqrt_norm(hid_ref[...].astype(F32))
        normed = (gain_ref[...] * x_hat).astype(BF16)
        nb[...] = normed
        nf_ref[...] = normed.astype(F32)
        m_s[...] = jnp.full_like(m_s, -jnp.inf)
        s_s[...] = jnp.zeros_like(s_s)
        l_s[...] = jnp.zeros_like(l_s)

    logits = LOGIT_SCALE * dot_nt(emb_ref[...], nb[...])
    ids = lax.broadcasted_iota(jnp.int32, (VT, TOK), 0) + row_start(i)
    hit = ids == lab_ref[...] - vp_ref[0] * VLOC
    fresh = ids >= i * VT
    masked = jnp.where(fresh, logits, -jnp.inf).reshape(VT // 8, 8, TOK)
    top = jnp.maximum(m_s[...], jnp.max(masked, axis=0))
    s_s[...] = s_s[...] * jnp.exp(m_s[...] - top) + jnp.sum(jnp.exp(masked - top[None]), axis=0)
    m_s[...] = top
    picked = jnp.where(jnp.logical_and(hit, fresh), logits, 0.0).reshape(VT // 8, 8, TOK)
    l_s[...] += jnp.sum(picked, axis=0)

    @pl.when(i == pl.num_programs(0) - 1)
    def _():
        row_m = jnp.max(m_s[...], axis=0, keepdims=True)
        row_s = jnp.sum(s_s[...] * jnp.exp(m_s[...] - row_m), axis=0, keepdims=True)
        row_l = jnp.sum(l_s[...], axis=0, keepdims=True)
        zeros = jnp.zeros((3, TOK), F32)
        st_ref[...] = jnp.concatenate([row_m, row_s, row_l, mask_ref[...], lab_ref[...].astype(F32), zeros], axis=0)


def own_stats(vp, hidden, gain, labels, mask, emb):
    whole = lambda shape: pl.BlockSpec(shape, lambda i, v: (0,) * len(shape))
    return pl.pallas_call(
        stats_kernel,
        grid_spec=pltpu.PrefetchScalarGridSpec(
            num_scalar_prefetch=1,
            grid=(NVT,),
            in_specs=[
                whole((TOK, WIDTH)),
                whole((1, WIDTH)),
                whole((1, TOK)),
                whole((1, TOK)),
                pl.BlockSpec((pl.Element(VT), pl.Element(WIDTH)), lambda i, v: (row_start(i), 0)),
            ],
            out_specs=[whole((TOK, WIDTH)), whole((8, TOK))],
            scratch_shapes=[pltpu.VMEM((TOK, WIDTH), BF16)] + [pltpu.VMEM((8, TOK), F32)] * 3,
        ),
        out_shape=[jax.ShapeDtypeStruct((TOK, WIDTH), F32), jax.ShapeDtypeStruct((8, TOK), F32)],
        compiler_params=pltpu.CompilerParams(dimension_semantics=("arbitrary",), vmem_limit_bytes=VMEM_LIMIT),
        name="own_stats",
    )(vp, hidden, gain, labels, mask, emb)


STEP = {"z+": (1, 0), "z-": (-1, 0), "y+": (0, 1), "y-": (0, -1)}


def tree_first():
    lo, mid, hi = 0, SPLIT // 2, SPLIT
    msgs = [
        dict(a=0, b=1, lo=lo, hi=hi, link="y+", parents=[]),
        dict(a=0, b=-1, lo=lo, hi=hi, link="y-", parents=[]),
        dict(a=0, b=2, lo=lo, hi=mid, link="y+", parents=[0]),
        dict(a=0, b=-2, lo=mid, hi=hi, link="y-", parents=[1]),
    ]
    for sign, link, part in ((1, "z+", (0, 2)), (-1, "z-", (2, 2))):
        for s in (1, 2, 3, 4):
            parents = [0, 1, 2, 3] if s == 1 else [len(msgs) - 1]
            msgs.append(dict(a=sign * s, b=(0, 4) if s < 4 else part, lo=lo, hi=hi, link=link, parents=parents))
    return msgs


def tree_second():
    lo, mid, hi = SPLIT, (SPLIT + TOK) // 2, TOK
    msgs = []
    nodes = [(0, lo, hi, None)]
    for sign, link, half in ((1, "z+", (lo, mid)), (-1, "z-", (mid, hi))):
        for s in (1, 2, 3, 4):
            rows = (lo, hi) if s < 4 else half
            parents = [] if s == 1 else [len(msgs) - 1]
            msgs.append(dict(a=sign * s, b=0, lo=rows[0], hi=rows[1], link=link, parents=parents))
            nodes.append((sign * s, rows[0], rows[1], len(msgs) - 1))
    for a, first, last, node in nodes:
        parents = [] if node is None else [node]
        up, down = len(msgs), len(msgs) + 1
        msgs.append(dict(a=a, b=1, lo=first, hi=last, link="y+", parents=parents))
        msgs.append(dict(a=a, b=-1, lo=first, hi=last, link="y-", parents=parents))
        if abs(a) < 4:
            msgs.append(dict(a=a, b=2, lo=lo, hi=mid, link="y+", parents=[up]))
            msgs.append(dict(a=a, b=-2, lo=mid, hi=hi, link="y-", parents=[down]))
        elif a == 4:
            msgs.append(dict(a=a, b=2, lo=first, hi=last, link="y+", parents=[up]))
        else:
            msgs.append(dict(a=a, b=-2, lo=first, hi=last, link="y-", parents=[down]))
    return msgs


def arrival_order(msgs):
    size = lambda m: (m["hi"] - m["lo"]) * (m["b"][1] if isinstance(m["b"], tuple) else 1)
    free = {link: 0.0 for link in STEP}
    waiting = {i: set(m["parents"]) for i, m in enumerate(msgs)}
    heap, order = [], []

    def push(i, now):
        link = msgs[i]["link"]
        free[link] = max(free[link], now) + size(msgs[i]) * WIDTH * 4 / 60e3
        heapq.heappush(heap, (free[link] + 2.0, i))

    for i in range(len(msgs)):
        if not waiting[i]:
            push(i, 0.0)
    while heap:
        now, i = heapq.heappop(heap)
        order.append(i)
        for j in range(len(msgs)):
            if i in waiting[j]:
                waiting[j].discard(i)
                if not waiting[j]:
                    push(j, now)
    return order


FIRST, SECOND = tree_first(), tree_second()
NMSG = max(len(FIRST), len(SECOND))


def peers():
    dp, vp = lax.axis_index("dp"), lax.axis_index("vp")
    z, y = lax.div(dp, NY), lax.rem(dp, NY)
    ys = [z * NY + lax.rem(y + d, NY) for d in range(1, NY)]
    zs = [lax.rem(z + d, NZ) * NY + y for d in range(1, NZ)]
    vs = [lax.rem(vp + d, NV) for d in range(1, NV)]
    return dp, vp, z, y, ys, zs, vs


def greet(dp, vp, ys, zs, vs):
    barrier = pltpu.get_barrier_semaphore()
    everyone = [(d, vp) for d in ys + zs] + [(dp, v) for v in vs]
    for device in everyone:
        pl.semaphore_signal(barrier, inc=1, device_id=device, device_id_type=MESH)
    pl.semaphore_wait(barrier, len(everyone))


def remote(src, dst, send, recv, device):
    return pltpu.make_async_remote_copy(
        src_ref=src, dst_ref=dst, send_sem=send, recv_sem=recv, device_id=device, device_id_type=MESH
    )


def gather_kernel(nf_ref, st_ref, nall_ref, stall_ref, vbuf, stbuf, local, sent, got, twin, st_sent, st_got):
    dp, vp, z, y, ys, zs, vs = peers()
    core = lax.rem(vp, 2)
    other = vp + 1 - 2 * core
    greet(dp, vp, ys, zs, vs)

    def region(m, dz=0, dy=0):
        zz = lax.rem(z - m["a"] + dz + 2 * NZ, NZ)
        rows = pl.ds(m["lo"], m["hi"] - m["lo"])
        if isinstance(m["b"], tuple):
            return nall_ref.at[zz, pl.ds(*m["b"]), rows]
        return nall_ref.at[zz, lax.rem(y - m["b"] + dy + 2 * NY, NY), rows]

    def target(link, back=False):
        dz, dy = STEP[link]
        if back:
            dz, dy = -dz, -dy
        return (lax.rem(z + dz + NZ, NZ) * NY + lax.rem(y + dy + NY, NY), vp)

    def send(m, i, mine):
        dz, dy = STEP[m["link"]]
        place = region(m, dz, dy)
        src = nf_ref.at[pl.ds(m["lo"], m["hi"] - m["lo"])] if mine else place
        copy = remote(src, place, sent.at[i], got.at[i], target(m["link"]))
        copy.start()
        return copy

    own = pltpu.make_async_copy(nf_ref, nall_ref.at[z, y], local)
    own.start()
    for which, msgs in ((0, FIRST), (1, SECOND)):

        @pl.when(core == which)
        def _():
            for i, m in enumerate(msgs):
                if not m["parents"]:
                    send(m, i, True)

    vbuf[vp] = st_ref[...]
    stat_copies = [
        remote(st_ref, vbuf.at[vp], st_sent.at[i], st_got.at[i], (dp, v)) for i, v in enumerate(vs)
    ]
    for copy in stat_copies:
        copy.start()
    for i, v in enumerate(vs):
        source = lax.rem(vp + NV - 1 - i, NV)
        remote(st_ref, vbuf.at[source], st_sent.at[i], st_got.at[i], (dp, v)).wait_recv()
    row_m = vbuf[0, 0:1]
    for p in range(1, NV):
        row_m = jnp.maximum(row_m, vbuf[p, 0:1])
    row_s = jnp.zeros_like(row_m)
    row_l = jnp.zeros_like(row_m)
    for p in range(NV):
        row_s += vbuf[p, 1:2] * jnp.exp(vbuf[p, 0:1] - row_m)
        row_l += vbuf[p, 2:3]
    lse = row_m + jnp.log(row_s)
    lanes = lambda d, n=1: pl.ds(pl.multiple_of(d * TOK, TOK), n * TOK)
    stbuf[:, lanes(dp)] = jnp.concatenate([lse, st_ref[3:5], row_l, jnp.zeros((4, TOK), F32)], axis=0)
    for i, d in enumerate(ys):
        copy = remote(stbuf.at[:, lanes(dp)], stbuf.at[:, lanes(dp)], st_sent.at[7 + i], st_got.at[7 + i], (d, vp))
        copy.start()
        stat_copies.append(copy)
    for i, d in enumerate(ys):
        source = z * NY + lax.rem(y + NY - 1 - i, NY)
        place = stbuf.at[:, lanes(source)]
        remote(place, place, st_sent.at[7 + i], st_got.at[7 + i], (d, vp)).wait_recv()
    for i, d in enumerate(zs):
        place = stbuf.at[:, lanes(z * NY, NY)]
        copy = remote(place, place, st_sent.at[10 + i], st_got.at[10 + i], (d, vp))
        copy.start()
        stat_copies.append(copy)

    own.wait()
    for which, msgs, others in ((0, FIRST, SECOND), (1, SECOND, FIRST)):

        @pl.when(core == which)
        def _():
            ready = set()
            copies = []
            for i, m in enumerate(msgs):
                if not m["parents"]:
                    place = region(m, *STEP[m["link"]])
                    src = nf_ref.at[pl.ds(m["lo"], m["hi"] - m["lo"])]
                    copies.append(remote(src, place, sent.at[i], got.at[i], target(m["link"])))
            for i in arrival_order(msgs):
                m = msgs[i]
                place = region(m)
                remote(place, place, sent.at[i], got.at[i], target(m["link"], True)).wait_recv()
                ready.add(i)
                for j, child in enumerate(msgs):
                    if i in child["parents"] and ready.issuperset(child["parents"]):
                        copies.append(send(child, j, False))
                copy = remote(place, place, sent.at[NMSG + i], twin.at[i], (dp, other))
                copy.start()
                copies.append(copy)
            for i, m in enumerate(others):
                place = region(m)
                remote(place, place, sent.at[i], twin.at[i], (dp, other)).wait_recv()
            for copy in copies:
                copy.wait_send()

    for i, d in enumerate(zs):
        source = lax.rem(z + NZ - 1 - i, NZ)
        place = stbuf.at[:, lanes(source * NY, NY)]
        remote(place, place, st_sent.at[10 + i], st_got.at[10 + i], (d, vp)).wait_recv()
    for copy in stat_copies:
        copy.wait_send()
    stall_ref[...] = stbuf[...]


def gather(nf, st):
    any_space = pl.BlockSpec(memory_space=pl.ANY)
    vmem = pl.BlockSpec(memory_space=pltpu.VMEM)
    return pl.pallas_call(
        gather_kernel,
        in_specs=[vmem, vmem],
        out_specs=[any_space, vmem],
        out_shape=[jax.ShapeDtypeStruct((NZ, NY, TOK, WIDTH), F32), jax.ShapeDtypeStruct((8, NALL), F32)],
        scratch_shapes=[
            pltpu.VMEM((NV, 8, TOK), F32),
            pltpu.VMEM((8, NALL), F32),
            pltpu.SemaphoreType.DMA,
            pltpu.SemaphoreType.DMA((2 * NMSG,)),
            pltpu.SemaphoreType.DMA((NMSG,)),
            pltpu.SemaphoreType.DMA((NMSG,)),
            pltpu.SemaphoreType.DMA((17,)),
            pltpu.SemaphoreType.DMA((17,)),
        ],
        compiler_params=pltpu.CompilerParams(
            collective_id=0, has_side_effects=True, vmem_limit_bytes=VMEM_LIMIT
        ),
        name="gather_tokens",
    )(nf, st)


def weight_scale(st_ref):
    return LOGIT_SCALE / jnp.sum(st_ref[1:2, :])


def dn_kernel(ids_ref, nf_ref, st_ref, own_ref, emb_ref, dn_ref, w_s):
    i = pl.program_id(0)

    @pl.when(i == 0)
    def _():
        w_s[...] = own_ref[1:2, :] * weight_scale(st_ref)
        dn_ref[...] = jnp.zeros_like(dn_ref)

    emb = emb_ref[...]
    logits = LOGIT_SCALE * dot_nt(emb, nf_ref[...].astype(BF16))
    ids = lax.broadcasted_iota(jnp.int32, (VT, TOK), 0) + row_start(i)
    soft = jnp.exp(logits - own_ref[0:1, :])
    hit = ids == own_ref[2:3, :].astype(jnp.int32) - ids_ref[1] * VLOC
    weight = jnp.where(ids >= i * VT, w_s[...], 0.0)
    d_logits = (jnp.where(hit, soft - 1.0, soft) * weight).astype(BF16)
    dn_ref[...] += lax.dot_general(d_logits, emb, (((0,), (0,)), ((), ())), preferred_element_type=F32)


def own_dn(ids, nf, stall, emb):
    whole = lambda shape: pl.BlockSpec(shape, lambda i, v: (0,) * len(shape))
    return pl.pallas_call(
        dn_kernel,
        grid_spec=pltpu.PrefetchScalarGridSpec(
            num_scalar_prefetch=1,
            grid=(NVT,),
            in_specs=[
                whole((TOK, WIDTH)),
                whole((8, NALL)),
                pl.BlockSpec((8, TOK), lambda i, v: (0, v[0])),
                pl.BlockSpec((pl.Element(VT), pl.Element(WIDTH)), lambda i, v: (row_start(i), 0)),
            ],
            out_specs=whole((TOK, WIDTH)),
            scratch_shapes=[pltpu.VMEM((1, TOK), F32)],
        ),
        out_shape=jax.ShapeDtypeStruct((TOK, WIDTH), F32),
        compiler_params=pltpu.CompilerParams(dimension_semantics=("arbitrary",), vmem_limit_bytes=VMEM_LIMIT),
        name="own_dn",
    )(ids, nf, stall, stall, emb)


def table_kernel(
    nall_ref, st_ref, emb_ref, dn_ref, hid_ref, gain_ref, table_ref, dh_ref, dg_ref, loss_ref,
    nb, stage, ebuf, acc, rows, dnbuf, dhbuf, gv, gy, gz,
    stage_sem, e_sem, l_sem, sent, got, v_sent, v_got,
):
    dp, vp, z, y, ys, zs, vs = peers()
    greet(dp, vp, ys, zs, vs)
    color_a = lax.rem(y + 2 * z, 4)
    color_b = lax.rem(z + 2 * y, 4)

    def a_row(color, k, start=0):
        return pl.multiple_of(color * COLOR_ROWS + k * CHUNK + start, HALF)

    def b_row(color, k, start=0):
        return pl.multiple_of(B_BASE + color * COLOR_ROWS + k * CHUNK + start, HALF)

    def fetch_rows(k, slot):
        return [
            pltpu.make_async_copy(
                emb_ref.at[pl.ds(a_row(color_a, k), CHUNK)], ebuf.at[slot, pl.ds(0, CHUNK)], e_sem.at[slot, 0]
            ),
            pltpu.make_async_copy(
                emb_ref.at[pl.ds(b_row(color_b, k), CHUNK)], ebuf.at[slot, pl.ds(CHUNK, CHUNK)], e_sem.at[slot, 1]
            ),
        ]

    def fetch_rest(part, slot):
        start, size = REST_PARTS[part]
        return pltpu.make_async_copy(
            emb_ref.at[pl.ds(start, size)], ebuf.at[slot, pl.ds(0, size)], e_sem.at[slot, 0]
        )

    def fetch_tokens(t, slot):
        return pltpu.make_async_copy(nall_ref.at[pl.ds(t * TT, TT)], stage.at[slot], stage_sem.at[slot])

    for copy in fetch_rows(0, 0):
        copy.start()
    fetch_tokens(0, 0).start()

    def part(v):
        return pl.ds(pl.multiple_of(v * SLICE, SLICE), SLICE)

    def dn_copy(i, v):
        return remote(dn_ref.at[part(v)], dnbuf.at[vp], v_sent.at[i], v_got.at[i], (dp, v))

    for i, v in enumerate(vs):
        dn_copy(i, v).start()

    count = jnp.sum(st_ref[1:2, :])
    rows[0:1] = st_ref[0:1, :]
    rows[1:2] = st_ref[1:2, :] * (LOGIT_SCALE / count)
    rows[2:3] = st_ref[2:3, :] - (vp * VLOC).astype(F32)
    loss_ref[0, 0] = jnp.sum(st_ref[1:2, :] * (st_ref[0:1, :] - st_ref[3:4, :])) / count

    def block(slot, rows_in, t, size, ids):
        tok = pl.ds(pl.multiple_of(t * TT, TT), TT)
        n = nb[tok, :]
        logits = LOGIT_SCALE * dot_nt(ebuf[rows_in, 0:size], n)
        soft = jnp.exp(logits - rows[0:1, tok])
        hit = ids == rows[2:3, tok].astype(jnp.int32)
        d_logits = (jnp.where(hit, soft - 1.0, soft) * rows[1:2, tok]).astype(BF16)
        acc[slot, 0:size] += jnp.dot(d_logits, n, preferred_element_type=F32)

    up_y, down_y = (ys[0], vp), (ys[2], vp)
    up_z, down_z = (zs[0], vp), (zs[6], vp)

    def row_copies(k, slot, ca, cb):
        a0, b0 = 0, CHUNK
        plan = [
            (a0, CHUNK, a_row(ca["y+"], k), up_y),
            (a0, CHUNK, a_row(ca["y-"], k), down_y),
            (a0, HALF, a_row(ca["z+"], k), up_z),
            (a0 + HALF, HALF, a_row(ca["z-"], k, HALF), down_z),
            (b0, CHUNK, b_row(cb["z+"], k), up_z),
            (b0, CHUNK, b_row(cb["z-"], k), down_z),
            (b0, HALF, b_row(cb["y+"], k), up_y),
            (b0 + HALF, HALF, b_row(cb["y-"], k, HALF), down_y),
        ]
        return [
            remote(acc.at[slot, pl.ds(lo, n)], table_ref.at[pl.ds(row, n)], sent.at[slot, i], got.at[k, i], device)
            for i, (lo, n, row, device) in enumerate(plan)
        ]

    def out_copies(k, slot):
        mine_a = dict.fromkeys(STEP, color_a)
        mine_b = dict.fromkeys(STEP, color_b)
        return row_copies(k, slot, mine_a, mine_b)

    def in_copies(k):
        from_a = {"y+": lax.rem(color_a + 3, 4), "y-": lax.rem(color_a + 1, 4)}
        from_a["z+"] = from_a["z-"] = lax.rem(color_a + 2, 4)
        from_b = {"z+": lax.rem(color_b + 3, 4), "z-": lax.rem(color_b + 1, 4)}
        from_b["y+"] = from_b["y-"] = lax.rem(color_b + 2, 4)
        return row_copies(k, 0, from_a, from_b)

    def keep_copies(k, slot):
        return [
            pltpu.make_async_copy(
                acc.at[slot, pl.ds(0, CHUNK)], table_ref.at[pl.ds(a_row(color_a, k), CHUNK)], l_sem.at[slot, 0]
            ),
            pltpu.make_async_copy(
                acc.at[slot, pl.ds(CHUNK, CHUNK)], table_ref.at[pl.ds(b_row(color_b, k), CHUNK)], l_sem.at[slot, 1]
            ),
        ]

    def dh_copy(i, v):
        return remote(dhbuf.at[part(vp)], dhbuf.at[part(vp)], v_sent.at[7 + i], v_got.at[7 + i], (dp, v))

    def gv_copy(i, v):
        return remote(gv.at[vp], gv.at[vp], v_sent.at[14 + i], v_got.at[14 + i], (dp, v))

    def gy_copy(i, d):
        return remote(gy.at[y], gy.at[y], v_sent.at[21 + i], v_got.at[21 + i], (d, vp))

    def gz_copy(i, d):
        return remote(gz.at[z], gz.at[z], v_sent.at[24 + i], v_got.at[24 + i], (d, vp))

    def total(buf, n):
        value = buf[0]
        for p in range(1, n):
            value += buf[p]
        return value

    def norm_backward():
        for i, v in enumerate(vs):
            source = lax.rem(vp + NV - 1 - i, NV)
            remote(dn_ref.at[part(v)], dnbuf.at[source], v_sent.at[i], v_got.at[i], (dp, v)).wait_recv()
        dnbuf[vp] = dn_ref[part(vp), :]
        d_normed = total(dnbuf, NV)
        x_hat, inv_std = rsqrt_norm(hid_ref[part(vp), :].astype(F32))
        value = d_normed * gain_ref[...]
        mean_one = jnp.mean(value, axis=-1, keepdims=True)
        mean_two = jnp.mean(value * x_hat, axis=-1, keepdims=True)
        dhbuf[part(vp), :] = (inv_std * (value - mean_one - x_hat * mean_two)).astype(BF16).astype(F32)
        gain_part = jnp.sum(d_normed * x_hat, axis=0, keepdims=True)
        gv[vp] = jnp.broadcast_to(gain_part, (8, WIDTH))
        for i, v in enumerate(vs):
            dh_copy(i, v).start()
            gv_copy(i, v).start()

    def hidden_out():
        for i, v in enumerate(vs):
            source = lax.rem(vp + NV - 1 - i, NV)
            place = dhbuf.at[part(source)]
            remote(place, place, v_sent.at[7 + i], v_got.at[7 + i], (dp, v)).wait_recv()
            remote(gv.at[source], gv.at[source], v_sent.at[14 + i], v_got.at[14 + i], (dp, v)).wait_recv()
        dh_ref[...] = dhbuf[...].astype(BF16)
        gy[y] = total(gv, NV)
        for i, d in enumerate(ys):
            gy_copy(i, d).start()

    def gain_y():
        for i, d in enumerate(ys):
            source = lax.rem(y + NY - 1 - i, NY)
            remote(gy.at[source], gy.at[source], v_sent.at[21 + i], v_got.at[21 + i], (d, vp)).wait_recv()
        gz[z] = total(gy, NY)
        for i, d in enumerate(zs):
            gz_copy(i, d).start()

    def gain_z():
        for i, d in enumerate(zs):
            source = lax.rem(z + NZ - 1 - i, NZ)
            remote(gz.at[source], gz.at[source], v_sent.at[24 + i], v_got.at[24 + i], (d, vp)).wait_recv()
        dg_ref[...] = total(gz, NZ)[0:1]

    def free(k, slot):
        for copy in out_copies(k, slot):
            copy.wait_send()
        for copy in keep_copies(k, slot):
            copy.wait()

    def chunk_step(k, carry):
        slot, rows_in = lax.rem(k, SLOTS), lax.rem(k, 2)
        for copy in fetch_rows(k, rows_in):
            copy.wait()

        @pl.when(k + 1 < NCHUNK)
        def _():
            for copy in fetch_rows(k + 1, 1 - rows_in):
                copy.start()

        @pl.when(k + 1 == NCHUNK)
        def _():
            fetch_rest(0, 1 - rows_in).start()

        @pl.when(k >= SLOTS)
        def _():
            free(k - SLOTS, slot)

        for step, work in ((1, norm_backward), (2, hidden_out), (3, gain_y), (4, gain_z)):
            pl.when(k == step)(work)

        acc[slot] = jnp.zeros((2 * CHUNK, WIDTH), F32)
        place = lax.broadcasted_iota(jnp.int32, (2 * CHUNK, 1), 0)
        ids = place + jnp.where(place < CHUNK, a_row(color_a, k), b_row(color_b, k) - CHUNK)

        def token_step(t, carry):
            @pl.when(k == 0)
            def _():
                half = lax.rem(t, 2)
                fetch_tokens(t, half).wait()

                @pl.when(t + 1 < NT)
                def _():
                    fetch_tokens(t + 1, 1 - half).start()

                nb[pl.ds(pl.multiple_of(t * TT, TT), TT), :] = stage[half].astype(BF16)

            block(slot, rows_in, t, 2 * CHUNK, ids)
            return carry

        lax.fori_loop(0, NT, token_step, 0)
        for copy in out_copies(k, slot) + keep_copies(k, slot):
            copy.start()
        return carry

    lax.fori_loop(0, NCHUNK, chunk_step, 0)

    rest_copies = []
    for p, (start, size) in enumerate(REST_PARTS):
        slot, rows_in = (NCHUNK + p) % SLOTS, (NCHUNK + p) % 2
        fetch_rest(p, rows_in).wait()
        if p + 1 < len(REST_PARTS):
            fetch_rest(p + 1, 1 - rows_in).start()
        free(NCHUNK + p - SLOTS, slot)
        acc[slot] = jnp.zeros((2 * CHUNK, WIDTH), F32)
        ids = lax.broadcasted_iota(jnp.int32, (size, 1), 0) + start

        def rest_step(t, carry):
            block(slot, rows_in, t, size, ids)
            return carry

        lax.fori_loop(0, NT, rest_step, 0)
        copy = pltpu.make_async_copy(acc.at[slot, pl.ds(0, size)], table_ref.at[pl.ds(start, size)], l_sem.at[slot, 0])
        copy.start()
        rest_copies.append(copy)

    free(NCHUNK - 1, (NCHUNK - 1) % SLOTS)
    for copy in rest_copies:
        copy.wait()

    def drain(k, carry):
        for copy in in_copies(k):
            copy.wait_recv()
        return carry

    lax.fori_loop(0, NCHUNK, drain, 0)
    for i, v in enumerate(vs):
        dn_copy(i, v).wait_send()
        dh_copy(i, v).wait_send()
        gv_copy(i, v).wait_send()
    for i, d in enumerate(ys):
        gy_copy(i, d).wait_send()
    for i, d in enumerate(zs):
        gz_copy(i, d).wait_send()


def table_grad(nall, stall, emb, dn, hidden, gain):
    any_space = pl.BlockSpec(memory_space=pl.ANY)
    vmem = pl.BlockSpec(memory_space=pltpu.VMEM)
    smem = pl.BlockSpec(memory_space=pltpu.SMEM)
    return pl.pallas_call(
        table_kernel,
        in_specs=[any_space, vmem, any_space, vmem, vmem, vmem],
        out_specs=[any_space, vmem, vmem, smem],
        out_shape=[
            jax.ShapeDtypeStruct((VLOC, WIDTH), F32),
            jax.ShapeDtypeStruct((TOK, WIDTH), BF16),
            jax.ShapeDtypeStruct((1, WIDTH), F32),
            jax.ShapeDtypeStruct((1, 1), F32),
        ],
        scratch_shapes=[
            pltpu.VMEM((NALL, WIDTH), BF16),
            pltpu.VMEM((2, TT, WIDTH), F32),
            pltpu.VMEM((2, 2 * CHUNK, WIDTH), BF16),
            pltpu.VMEM((SLOTS, 2 * CHUNK, WIDTH), F32),
            pltpu.VMEM((8, NALL), F32),
            pltpu.VMEM((NV, SLICE, WIDTH), F32),
            pltpu.VMEM((TOK, WIDTH), F32),
            pltpu.VMEM((NV, 8, WIDTH), F32),
            pltpu.VMEM((NY, 8, WIDTH), F32),
            pltpu.VMEM((NZ, 8, WIDTH), F32),
            pltpu.SemaphoreType.DMA((2,)),
            pltpu.SemaphoreType.DMA((2, 2)),
            pltpu.SemaphoreType.DMA((SLOTS, 2)),
            pltpu.SemaphoreType.DMA((SLOTS, 8)),
            pltpu.SemaphoreType.DMA((NCHUNK, 8)),
            pltpu.SemaphoreType.DMA((31,)),
            pltpu.SemaphoreType.DMA((31,)),
        ],
        compiler_params=pltpu.CompilerParams(
            collective_id=1, has_side_effects=True, vmem_limit_bytes=VMEM_LIMIT
        ),
        name="table_grad",
    )(nall, stall, emb, dn, hidden, gain)


def solution(mesh):
    def local_step(hidden, norm_gain, emb_table, labels, tok_mask):
        rows, seq_len, width = hidden.shape
        flat = hidden.reshape(rows * seq_len, width)
        gain = norm_gain.reshape(1, width)
        ids = jnp.stack([lax.axis_index("dp"), lax.axis_index("vp")]).astype(jnp.int32)
        nf, st = own_stats(ids[1:], flat, gain, labels.reshape(1, -1), tok_mask.reshape(1, -1), emb_table)
        nall, stall = gather(nf, st)
        dn = own_dn(ids, nf, stall, emb_table)
        table, d_hidden, d_gain, loss = table_grad(nall.reshape(NALL, width), stall, emb_table, dn, flat, gain)
        return loss[0, 0], table, d_hidden.reshape(rows, seq_len, width), d_gain[0]

    return jax.shard_map(
        local_step,
        mesh=mesh,
        in_specs=(P("dp", None, None), P(None), P("vp", None), P("dp", None), P("dp", None)),
        out_specs=(P(), P("vp", None), P("dp", None, None), P(None)),
        check_vma=False,
    )
```

```python
import jax
import jax.numpy as jnp
from jax import lax
from jax.experimental import pallas as pl
from jax.experimental.pallas import tpu as pltpu
from jax.sharding import PartitionSpec as P

MESH = pl.DeviceIdType.MESH
LOGIT_SCALE = 0.0625
EPS = 1e-5
NZ, NY, NV = 8, 4, 8
NDP = NZ * NY
TOK, WIDTH, VLOC = 384, 896, 18992
NALL = NDP * TOK
F32, BF16 = jnp.float32, jnp.bfloat16

ROWS_0, ROWS_1 = 112, 144
Q_BASE = ROWS_0 + ROWS_1
Q_ROWS = (TOK - Q_BASE) // NY
Q_PART = TOK - Q_BASE

COLOR_ROWS, CHUNK = 2304, 192
HALF, PAIR = CHUNK // 2, 2 * CHUNK
NCHUNK = COLOR_ROWS // CHUNK
B_BASE = NY * COLOR_ROWS
REST_BASE = 2 * B_BASE
REST_PARTS = ((REST_BASE, 288), (REST_BASE + 288, VLOC - REST_BASE - 288))
SLOTS = 3

TT = 2048
NT = NALL // TT
TILE = NY * Q_BASE
NQ = NDP * Q_PART // TILE
VT, VPARTS = 1184, ((0, 304), (304, 304), (608, 288), (896, 288))
NVT = VLOC // VT
VTAIL = VLOC - NVT * VT
NSTEP = 2 * NVT
SLICE = TOK // NV


def dot_nt(a, b):
    return lax.dot_general(a, b, (((1,), (1,)), ((), ())), preferred_element_type=F32)


def rsqrt_norm(values):
    mean_x = jnp.mean(values, axis=-1, keepdims=True)
    centered = values - mean_x
    variance = jnp.mean(centered * centered, axis=-1, keepdims=True)
    inv_std = lax.rsqrt(variance + EPS)
    return centered * inv_std, inv_std


STEP = {"z+": (1, 0, 0), "z-": (-1, 0, 0), "y+": (0, 1, 0), "y-": (0, -1, 0), "x+": (0, 0, 1), "x-": (0, 0, -1)}


def add(msgs, link, z, y, rows, parents, q):
    msgs.append(dict(link=link, z=z, y=y, lo=rows[0], hi=rows[1], parents=parents, q=q))
    return [len(msgs) - 1]


def halves(lo, hi):
    return (lo, (lo + hi) // 2), ((lo + hi) // 2, hi)


def ring(msgs, whole, last, roots, q=None):
    added = []
    for link, half in zip(("z+", "z-"), last):
        parents = roots
        for s in range(1, NZ // 2 + 1):
            y, rows = whole if 2 * s < NZ else half
            parents = add(msgs, link, s * STEP[link][0], y, rows, parents, q)
            added += parents
    return added


def fan(msgs, whole, last, roots, q=None):
    added = []
    for link, half in zip(("y+", "y-"), last):
        dy = STEP[link][1]
        first = add(msgs, link, whole[0], dy, whole[1], roots, q)
        added += first
        if half is not None:
            added += add(msgs, link, half[0], 2 * dy, half[1], first, q)
    return added


def tree_first():
    msgs = []
    every = ((0, NZ // 2), (NZ // 2, NZ // 2))
    rows = (0, Q_ROWS)
    column = ring(msgs, (0, rows), [(0, part) for part in halves(*rows)], [], 0)
    up, up_half, down, down_half = fan(msgs, ((0, NZ), rows), [(part, rows) for part in every], column, 0)
    for y, roots in ((0, column), (1, [up]), (-1, [down]), (2, [up_half, down_half])):
        for link, part in zip(("x+", "x-"), every):
            dx = STEP[link][2]
            first = add(msgs, link, (0, NZ), y, rows, roots, dx)
            add(msgs, link, part, y, rows, first, 2 * dx)
    rows = (0, ROWS_0)
    own = fan(msgs, (0, rows), [(0, part) for part in halves(*rows)], [])
    every = ((0, NY // 2), (NY // 2, NY // 2))
    ring(msgs, ((0, NY), rows), [(part, rows) for part in every], column + own)
    return msgs


def tree_second():
    msgs = []
    rows = (ROWS_0, Q_BASE)
    parts = halves(*rows)
    nodes = ring(msgs, (0, rows), [(0, part) for part in parts], [])
    fan(msgs, (0, rows), [(0, part) for part in parts], [])
    for i in nodes:
        z, whole = msgs[i]["z"], (msgs[i]["lo"], msgs[i]["hi"])
        fan(msgs, (z, whole), [(z, part) if whole in (rows, part) else None for part in parts], [i])
    return msgs


def plane(m):
    return m["z"] % NZ if m["q"] is None else None


PLANES = [0] + [d for s in range(1, NZ // 2) for d in (s, NZ - s)] + [NZ // 2]
EARLY = NZ - 3
UNITS = PLANES[:EARLY] + [None] * NQ + PLANES[EARLY:]


def length(span):
    return span[1] if isinstance(span, tuple) else 1


def schedule(trees):
    tick, latency, rate, now = 0.25, 2.0, 88e3, 7.0
    queues = {(link, core): [] for link in STEP for core in range(2)}
    missing = [[set(m["parents"]) for m in msgs] for msgs in trees]
    arrived = [[] for _ in trees]
    taken = [[[] for _ in range(NSTEP + len(UNITS) + 1)] for _ in trees]

    def push(core, i):
        m = trees[core][i]
        size = (m["hi"] - m["lo"]) * length(m["z"]) * length(m["y"]) * WIDTH * 4
        queues[m["link"], core].append([i, size])

    def advance():
        for link in STEP:
            busy = [core for core in range(2) if queues[link, core]]
            for core in busy:
                head = queues[link, core][0]
                head[1] -= rate * tick / len(busy)
                if head[1] <= 0:
                    queues[link, core].pop(0)
                    arrived[core].append((now + latency, head[0]))
        return now + tick

    def collect(slot, limit):
        for core in range(2):
            for item in sorted(arrived[core]):
                if item[0] <= limit:
                    arrived[core].remove(item)
                    taken[core][slot].append(item[1])
                    for j, wants in enumerate(missing[core]):
                        if item[1] in wants:
                            wants.discard(item[1])
                            if not wants:
                                push(core, j)

    def lacking(wanted):
        return any(
            wanted(m) and not any(i in group for group in taken[core])
            for core, msgs in enumerate(trees)
            for i, m in enumerate(msgs)
        )

    for core, msgs in enumerate(trees):
        for i, m in enumerate(msgs):
            if not m["parents"]:
                push(core, i)
    end = now + latency
    for step in range(NSTEP):
        end += 1.65 if step < NVT else 2.7
        while now < end:
            now = advance()
        collect(step, now - 0.5)
        if step == NVT - 1:
            end += 4.0
    for u, d in enumerate(UNITS):
        while now < end or lacking(lambda m: plane(m) == d):
            now = advance()
            if now >= end:
                collect(NSTEP + u, now)
        end = now + 2.5
    while lacking(lambda m: True):
        now = advance()
        if now >= end:
            collect(NSTEP + len(UNITS), now)
    return taken, now


TREES = (tree_first(), tree_second())
TAKEN, GATHER_TIME = schedule(TREES)
NMSG = max(map(len, TREES))


def peers():
    dp, vp = lax.axis_index("dp"), lax.axis_index("vp")
    z, y = lax.div(dp, NY), lax.rem(dp, NY)
    ys = [z * NY + lax.rem(y + d, NY) for d in range(1, NY)]
    zs = [lax.rem(z + d, NZ) * NY + y for d in range(1, NZ)]
    vs = [lax.rem(vp + d, NV) for d in range(1, NV)]
    return dp, vp, z, y, ys, zs, vs


def greet(dp, vp, ys, zs, vs):
    barrier = pltpu.get_barrier_semaphore()
    everyone = [(d, vp) for d in ys + zs] + [(dp, v) for v in vs]
    for device in everyone:
        pl.semaphore_signal(barrier, inc=1, device_id=device, device_id_type=MESH)
    pl.semaphore_wait(barrier, len(everyone))


def remote(src, dst, send, recv, device):
    return pltpu.make_async_remote_copy(
        src_ref=src, dst_ref=dst, send_sem=send, recv_sem=recv, device_id=device, device_id_type=MESH
    )


def lanes(d, n=1):
    return pl.ds(pl.multiple_of(d * TOK, TOK), n * TOK)


def part(v):
    return pl.ds(pl.multiple_of(v * SLICE, SLICE), SLICE)


def total(buf, n):
    value = buf[0]
    for p in range(1, n):
        value += buf[p]
    return value


class Exchange:
    def __init__(self, sent, got, devices, me, place, source=None):
        self.count, self.me = len(devices), me
        self.make = lambda i, at, to: remote(source[i] if source and to else place(at), place(at), sent.at[i], got.at[i], devices[i])

    def start(self):
        for i in range(self.count):
            self.make(i, self.me, True).start()

    def wait(self):
        n = self.count + 1
        for i in range(self.count):
            self.make(i, lax.rem(self.me + n - 1 - i, n), False).wait_recv()

    def drain(self):
        for i in range(self.count):
            self.make(i, self.me, True).wait_send()


def step_kernel(
    hid_ref, gain_ref, lab_ref, mask_ref, emb_ref, table_ref, nall_ref, dh_ref, dg_ref, loss_ref,
    nf, own, vbuf, ebuf, tailbuf, m_s, s_s, l_s, stat, own_row, lsebuf, maskbuf, rows,
    nb, stage, cbuf, acc, planes, dn, dnbuf, dhbuf, gv, gy, gz,
    local, e_sem, sent, got, twin, stage_sem, c_sem, l_sem, row_sent, row_got,
    stat_sem, mask_y, mask_z, lse_y, lse_z, dn_sem, dh_sem, gv_sem, gy_sem, gz_sem,
):
    dp, vp, z, y, ys, zs, vs = peers()
    x, core = lax.div(vp, 2), lax.rem(vp, 2)
    other = vp + 1 - 2 * core
    y_devices = [(d, vp) for d in ys]
    z_devices = [(d, vp) for d in zs]
    v_devices = [(dp, v) for v in vs]

    def fetch(step, slot):
        start = pl.multiple_of(lax.rem(step, NVT) * VT, 16)
        return pltpu.make_async_copy(emb_ref.at[pl.ds(start, VT)], ebuf.at[slot], e_sem.at[slot])

    tail = pltpu.make_async_copy(emb_ref.at[pl.ds(NVT * VT, VTAIL)], tailbuf, local.at[2])
    fetch(0, 0).start()
    tail.start()
    greet(dp, vp, ys, zs, vs)

    gain = gain_ref[...].reshape(1, WIDTH)
    x_hat, _ = rsqrt_norm(hid_ref[...].astype(F32))
    normed = (gain * x_hat).astype(BF16)
    own[...] = normed
    nf[...] = normed.astype(F32)
    m_s[...] = jnp.full_like(m_s, -jnp.inf)
    s_s[...] = jnp.zeros_like(s_s)
    l_s[...] = jnp.zeros_like(l_s)
    dn[...] = jnp.zeros_like(dn)
    labels = jnp.concatenate([lab_ref[i : i + 1] for i in range(3)], axis=1)
    mask = jnp.concatenate([mask_ref[i : i + 1] for i in range(3)], axis=1)
    own_row[0:1] = labels.astype(F32)
    maskbuf[:, lanes(dp)] = jnp.concatenate([mask, labels.astype(F32), jnp.zeros((6, TOK), F32)], axis=0)

    def box_rows(m, dx=0):
        if m["q"] is None:
            return pl.ds(m["lo"], m["hi"] - m["lo"])
        start = Q_BASE + Q_ROWS * lax.rem(x - m["q"] + dx + NV, NY) + m["lo"]
        return pl.ds(pl.multiple_of(start, 8), m["hi"] - m["lo"])

    def region(m, dz=0, dy=0, dx=0):
        zz = pl.ds(*m["z"]) if isinstance(m["z"], tuple) else lax.rem(z - m["z"] + dz + 2 * NZ, NZ)
        yy = pl.ds(*m["y"]) if isinstance(m["y"], tuple) else lax.rem(y - m["y"] + dy + 2 * NY, NY)
        return nall_ref.at[zz, yy, box_rows(m, dx)]

    def target(link, back=False):
        dz, dy, dx = [-d if back else d for d in STEP[link]]
        row = lax.rem(z + dz + NZ, NZ) * NY + lax.rem(y + dy + NY, NY)
        return (row, lax.rem(vp + 2 * dx + NV, NV))

    def out_copy(msgs, i):
        m = msgs[i]
        there = region(m, *STEP[m["link"]])
        src = there if m["parents"] else nf.at[box_rows(m)]
        return remote(src, there, sent.at[i], got.at[i], target(m["link"]))

    def twin_copy(msgs, i):
        here = region(msgs[i])
        return remote(here, here, sent.at[NMSG + i], twin.at[i], (dp, other))

    def per_core(work):
        for which in range(2):
            pl.when(core == which)(lambda: work(which))

    def take(which, k):
        msgs = TREES[which]
        done = set(i for group in TAKEN[which][:k] for i in group)
        for i in TAKEN[which][k]:
            here = region(msgs[i])
            remote(here, here, sent.at[i], got.at[i], target(msgs[i]["link"], True)).wait_recv()
            done.add(i)
            for j, child in enumerate(msgs):
                if i in child["parents"] and done.issuperset(child["parents"]):
                    out_copy(msgs, j).start()
            twin_copy(msgs, i).start()

    def take_twins(which, wanted):
        msgs = TREES[1 - which]
        for group in TAKEN[1 - which]:
            for i in group:
                if wanted(msgs[i]):
                    twin_copy(msgs, i).wait_recv()

    def roots(which):
        for i, m in enumerate(TREES[which]):
            if not m["parents"]:
                out_copy(TREES[which], i).start()

    def drain_gather(which):
        for i in range(len(TREES[which])):
            out_copy(TREES[which], i).wait_send()
            twin_copy(TREES[which], i).wait_send()

    q_own = pl.ds(pl.multiple_of(Q_BASE + Q_ROWS * x, 8), Q_ROWS)
    keep_own = [
        pltpu.make_async_copy(nf.at[place], nall_ref.at[z, y, place], local.at[i])
        for i, place in enumerate((pl.ds(0, Q_BASE), q_own))
    ]
    per_core(roots)
    for copy in keep_own:
        copy.start()

    def spread(buf, y_sem, z_sem):
        to_y = Exchange(y_sem.at[0], y_sem.at[1], y_devices, y, lambda at: buf.at[:, lanes(z * NY + at)])
        to_z = Exchange(z_sem.at[0], z_sem.at[1], z_devices, z, lambda at: buf.at[:, lanes(at * NY, NY)])
        return to_y, to_z

    def turn(pair):
        pair[0].wait()
        pair[1].start()

    masks = spread(maskbuf, mask_y, mask_z)
    lses = spread(lsebuf, lse_y, lse_z)
    stats = Exchange(stat_sem.at[0], stat_sem.at[1], v_devices, vp, lambda at: vbuf.at[at])
    dns = Exchange(
        dn_sem.at[0], dn_sem.at[1], v_devices, vp, lambda at: dnbuf.at[at], [dn.at[part(v)] for v in vs]
    )
    dhs = Exchange(dh_sem.at[0], dh_sem.at[1], v_devices, vp, lambda at: dhbuf.at[part(at)])
    gvs = Exchange(gv_sem.at[0], gv_sem.at[1], v_devices, vp, lambda at: gv.at[at])
    gys = Exchange(gy_sem.at[0], gy_sem.at[1], y_devices, y, lambda at: gy.at[at])
    gzs = Exchange(gz_sem.at[0], gz_sem.at[1], z_devices, z, lambda at: gz.at[at])

    masks[0].start()
    for copy in (*keep_own, tail):
        copy.wait()

    def tile_ids(start, size):
        return lax.broadcasted_iota(jnp.int32, (size, 1), 0) + start

    def own_labels():
        return own_row[0:1].astype(jnp.int32) - vp * VLOC

    def stats_rows(carry, emb, start):
        m, s, picked = carry
        size = emb.shape[0]
        logits = LOGIT_SCALE * dot_nt(emb, own[...])
        groups = lambda value: value.reshape(size // 8, 8, TOK)
        top = jnp.maximum(m, jnp.max(groups(logits), axis=0))
        s = s * jnp.exp(m - top) + jnp.sum(jnp.exp(groups(logits) - top[None]), axis=0)
        hit = tile_ids(start, size) == own_labels()
        return top, s, picked + jnp.sum(groups(jnp.where(hit, logits, 0.0)), axis=0)

    def stats_step(tile, slot):
        carry = (m_s[...], s_s[...], l_s[...])
        for lo, size in VPARTS:
            carry = stats_rows(carry, ebuf[slot, lo : lo + size], tile * VT + lo)
        m_s[...], s_s[...], l_s[...] = carry

    def stats_send():
        m_s[...], s_s[...], l_s[...] = stats_rows((m_s[...], s_s[...], l_s[...]), tailbuf[...], NVT * VT)
        row_m = jnp.max(m_s[...], axis=0, keepdims=True)
        row_s = jnp.sum(s_s[...] * jnp.exp(m_s[...] - row_m), axis=0, keepdims=True)
        row_l = jnp.sum(l_s[...], axis=0, keepdims=True)
        vbuf[vp] = jnp.concatenate([row_m, row_s, row_l, jnp.zeros((5, TOK), F32)], axis=0)
        stats.start()

    def stats_join():
        stats.wait()
        row_m = vbuf[0, 0:1]
        for p in range(1, NV):
            row_m = jnp.maximum(row_m, vbuf[p, 0:1])
        row_s = jnp.zeros_like(row_m)
        row_l = jnp.zeros_like(row_m)
        for p in range(NV):
            row_s += vbuf[p, 1:2] * jnp.exp(vbuf[p, 0:1] - row_m)
            row_l += vbuf[p, 2:3]
        lse = row_m + jnp.log(row_s)
        lsebuf[:, lanes(dp)] = jnp.concatenate([lse, row_l, jnp.zeros((6, TOK), F32)], axis=0)
        own_row[1:2] = lse
        own_row[2:3] = maskbuf[0:1, lanes(dp)] * (LOGIT_SCALE / jnp.sum(maskbuf[0:1]))
        lses[0].start()

    def dn_rows(emb, start):
        soft = jnp.exp(LOGIT_SCALE * dot_nt(emb, own[...]) - own_row[1:2])
        hit = tile_ids(start, emb.shape[0]) == own_labels()
        d_logits = (jnp.where(hit, soft - 1.0, soft) * own_row[2:3]).astype(BF16)
        return lax.dot_general(d_logits, emb, (((0,), (0,)), ((), ())), preferred_element_type=F32)

    def dn_step(tile, slot):
        dn[...] += dn_rows(ebuf[slot], tile * VT)

    actions = {
        5: lambda: turn(masks),
        NVT - 2: lambda: masks[1].wait(),
        NVT - 1: stats_send,
        NVT + 8: lambda: turn(lses),
    }

    def compute_step(step, carry):
        slot = lax.rem(step, 2)
        fetch(step, slot).wait()

        @pl.when(step + 1 < NSTEP)
        def _():
            fetch(step + 1, 1 - slot).start()

        @pl.when(step < NVT)
        def _():
            stats_step(step, slot)

        @pl.when(step >= NVT)
        def _():
            dn_step(step - NVT, slot)

        for k in range(NSTEP):

            @pl.when(step == k)
            def _():
                if k in actions:
                    actions[k]()
                per_core(lambda which: take(which, k))
                if k == NVT - 1:
                    stats_join()

        return carry

    lax.fori_loop(0, NSTEP, compute_step, 0)
    dn[...] += dn_rows(tailbuf[...], NVT * VT)
    lses[1].wait()

    count = jnp.sum(maskbuf[0:1])
    loss_ref[0, 0] = jnp.sum(maskbuf[0:1] * (lsebuf[0:1] - lsebuf[1:2])) / count
    weight, local_label = maskbuf[0:1] * (LOGIT_SCALE / count), maskbuf[1:2] - (vp * VLOC).astype(F32)
    stat[...] = jnp.concatenate([lsebuf[0:1], weight, local_label, jnp.zeros((5, NALL), F32)], axis=0)
    for d in range(NDP):
        first, shared = d * Q_BASE, NDP * Q_BASE + d * Q_PART
        rows[:, first : first + Q_BASE] = stat[:, d * TOK : d * TOK + Q_BASE]
        rows[:, shared : shared + Q_PART] = stat[:, d * TOK + Q_BASE : (d + 1) * TOK]
    dns.start()

    color_a = lax.rem(y + 2 * z, NY)
    color_b = lax.rem(z + 2 * y, NY)

    def a_row(color, k, start=0):
        return pl.multiple_of(color * COLOR_ROWS + k * CHUNK + start, HALF)

    def b_row(color, k, start=0):
        return pl.multiple_of(B_BASE + color * COLOR_ROWS + k * CHUNK + start, HALF)

    def fetch_rows(k, slot):
        return [
            pltpu.make_async_copy(emb_ref.at[pl.ds(row, CHUNK)], cbuf.at[slot, pl.ds(i * CHUNK, CHUNK)], c_sem.at[slot, i])
            for i, row in enumerate((a_row(color_a, k), b_row(color_b, k)))
        ]

    def fetch_rest(p, slot):
        start, size = REST_PARTS[p]
        return pltpu.make_async_copy(emb_ref.at[pl.ds(start, size)], cbuf.at[slot, pl.ds(0, size)], c_sem.at[slot, 0])

    def chunk_ids(k):
        place = lax.broadcasted_iota(jnp.int32, (PAIR, 1), 0)
        return place + jnp.where(place < CHUNK, a_row(color_a, k), b_row(color_b, k) - CHUNK)

    def block(rows_in, start, tokens, ids):
        tok = pl.ds(pl.multiple_of(start, tokens), tokens)
        n = nb[tok, :]
        logits = LOGIT_SCALE * dot_nt(cbuf[rows_in, : ids.shape[0]], n)
        soft = jnp.exp(logits - rows[0:1, tok])
        hit = ids == rows[2:3, tok].astype(jnp.int32)
        d_logits = (jnp.where(hit, soft - 1.0, soft) * rows[1:2, tok]).astype(BF16)
        return jnp.dot(d_logits, n, preferred_element_type=F32)

    up_y, down_y = y_devices[0], y_devices[-1]
    up_z, down_z = z_devices[0], z_devices[-1]

    def row_copies(k, slot, a_from, b_from):
        plan = [
            (0, CHUNK, a_row(a_from[0], k), up_y),
            (0, CHUNK, a_row(a_from[1], k), down_y),
            (0, HALF, a_row(a_from[2], k), up_z),
            (HALF, HALF, a_row(a_from[3], k, HALF), down_z),
            (CHUNK, CHUNK, b_row(b_from[2], k), up_z),
            (CHUNK, CHUNK, b_row(b_from[3], k), down_z),
            (CHUNK, HALF, b_row(b_from[0], k), up_y),
            (CHUNK + HALF, HALF, b_row(b_from[1], k, HALF), down_y),
        ]
        return [
            remote(acc.at[slot, pl.ds(lo, n)], table_ref.at[pl.ds(row, n)], row_sent.at[slot, i], row_got.at[k, i], device)
            for i, (lo, n, row, device) in enumerate(plan)
        ]

    def out_copies(k, slot):
        return row_copies(k, slot, [color_a] * 4, [color_b] * 4)

    def in_copies(k):
        near_a = [lax.rem(color_a + d, NY) for d in (3, 1, 2, 2)]
        near_b = [lax.rem(color_b + d, NY) for d in (2, 2, 3, 1)]
        return row_copies(k, 0, near_a, near_b)

    def keep_copies(k, slot):
        return [
            pltpu.make_async_copy(acc.at[slot, pl.ds(i * CHUNK, CHUNK)], table_ref.at[pl.ds(row, CHUNK)], l_sem.at[slot, i])
            for i, row in enumerate((a_row(color_a, k), b_row(color_b, k)))
        ]

    def send_rows(k, slot):
        for copy in out_copies(k, slot) + keep_copies(k, slot):
            copy.start()

    def free(k, slot):
        for copy in out_copies(k, slot):
            copy.wait_send()
        for copy in keep_copies(k, slot):
            copy.wait()

    for k in range(2):
        for copy in fetch_rows(k, k):
            copy.start()
    for copy in fetch_rows(0, 0):
        copy.wait()
    first_ids = chunk_ids(0)

    def plane_of(u):
        p = jnp.where(u < EARLY, u, u - NQ)
        step = lax.div(p + 1, 2)
        return lax.rem(z + jnp.where(lax.rem(p, 2) == 1, NZ - step, step), NZ)

    def shared(u):
        return jnp.logical_and(u >= EARLY, u < EARLY + NQ)

    def tile_start(u):
        start = jnp.where(shared(u), NDP * Q_BASE + (u - EARLY) * TILE, plane_of(u) * TILE)
        return pl.multiple_of(start, TILE)

    def stage_plane(u):
        return [
            pltpu.make_async_copy(
                nall_ref.at[plane_of(u), i, pl.ds(0, Q_BASE)], stage.at[pl.ds(i * Q_BASE, Q_BASE)], stage_sem.at[i]
            )
            for i in range(NY)
        ]

    def stage_shared(u):
        per = TILE // Q_PART
        return [
            pltpu.make_async_copy(
                nall_ref.at[(u - EARLY) * (per // NY) + i // NY, i % NY, pl.ds(Q_BASE, Q_PART)],
                stage.at[pl.ds(i * Q_PART, Q_PART)],
                stage_sem.at[i],
            )
            for i in range(per)
        ]

    def each_stage(u, work):
        for is_it, copies in ((shared(u), stage_shared), (jnp.logical_not(shared(u)), stage_plane)):

            @pl.when(jnp.logical_and(is_it, u < len(UNITS)))
            def _():
                for copy in copies(u):
                    work(copy)

    acc[0] = jnp.zeros((PAIR, WIDTH), F32)

    def unit_step(u, carry):
        for k, d in enumerate(UNITS):

            @pl.when(u == k)
            def _():
                def arrive(which):
                    take(which, NSTEP + k)
                    if k == 0 or UNITS[k - 1] != d:
                        take_twins(which, lambda m: plane(m) == d)

                per_core(arrive)

        each_stage(u, lambda copy: copy.start())
        before = u - 1

        @pl.when(jnp.logical_and(u > 0, jnp.logical_not(shared(before))))
        def _():
            planes[plane_of(before)] = block(0, tile_start(before), TILE, first_ids)

        @pl.when(shared(before))
        def _():
            acc[0] += block(0, tile_start(before), TILE, first_ids)

        each_stage(u, lambda copy: copy.wait())

        @pl.when(u < len(UNITS))
        def _():
            nb[pl.ds(tile_start(u), TILE), :] = stage[...].astype(BF16)

        return carry

    lax.fori_loop(0, len(UNITS) + 1, unit_step, 0)
    per_core(lambda which: take(which, NSTEP + len(UNITS)))
    acc[0] += total(planes, NZ)
    send_rows(0, 0)

    def norm_backward():
        dns.wait()
        dnbuf[vp] = dn[part(vp), :]
        d_normed = total(dnbuf, NV)
        x_hat, inv_std = rsqrt_norm(hid_ref[part(vp), :].astype(F32))
        value = d_normed * gain_ref[...].reshape(1, WIDTH)
        mean_one = jnp.mean(value, axis=-1, keepdims=True)
        mean_two = jnp.mean(value * x_hat, axis=-1, keepdims=True)
        dhbuf[part(vp), :] = (inv_std * (value - mean_one - x_hat * mean_two)).astype(BF16).astype(F32)
        gv[vp] = jnp.broadcast_to(jnp.sum(d_normed * x_hat, axis=0, keepdims=True), (8, WIDTH))
        dhs.start()
        gvs.start()

    def hidden_out():
        dhs.wait()
        gvs.wait()
        dh_ref[...] = dhbuf[...].astype(BF16)
        gy[y] = total(gv, NV)
        gys.start()

    def gain_z():
        gys.wait()
        gz[z] = total(gy, NY)
        gzs.start()

    def gain_out():
        gzs.wait()
        dg_ref[...] = total(gz, NZ)[0:1].reshape(WIDTH)

    def chunk_step(k, carry):
        slot, rows_in = lax.rem(k, SLOTS), lax.rem(k, 2)
        for copy in fetch_rows(k, rows_in):
            copy.wait()

        @pl.when(k + 1 < NCHUNK)
        def _():
            for copy in fetch_rows(k + 1, 1 - rows_in):
                copy.start()

        @pl.when(k + 1 == NCHUNK)
        def _():
            fetch_rest(0, 1 - rows_in).start()

        @pl.when(k >= SLOTS)
        def _():
            free(k - SLOTS, slot)

        for when, work in ((1, norm_backward), (2, hidden_out), (5, gain_z), (9, gain_out)):
            pl.when(k == when)(work)

        acc[slot] = jnp.zeros((PAIR, WIDTH), F32)
        ids = chunk_ids(k)

        def token_step(t, carry):
            acc[slot] += block(rows_in, t * TT, TT, ids)
            return carry

        lax.fori_loop(0, NT, token_step, 0)
        send_rows(k, slot)
        return carry

    lax.fori_loop(1, NCHUNK, chunk_step, 0)

    rest_copies = []
    for p, (start, size) in enumerate(REST_PARTS):
        slot, rows_in = (NCHUNK + p) % SLOTS, (NCHUNK + p) % 2
        fetch_rest(p, rows_in).wait()
        if p + 1 < len(REST_PARTS):
            fetch_rest(p + 1, 1 - rows_in).start()
        free(NCHUNK + p - SLOTS, slot)
        acc[slot] = jnp.zeros((PAIR, WIDTH), F32)
        ids = lax.broadcasted_iota(jnp.int32, (size, 1), 0) + start

        def rest_step(t, carry):
            acc[slot, :size] += block(rows_in, t * TT, TT, ids)
            return carry

        lax.fori_loop(0, NT, rest_step, 0)
        copy = pltpu.make_async_copy(acc.at[slot, pl.ds(0, size)], table_ref.at[pl.ds(start, size)], l_sem.at[slot, 0])
        copy.start()
        rest_copies.append(copy)

    free(NCHUNK - 1, (NCHUNK - 1) % SLOTS)
    for copy in rest_copies:
        copy.wait()

    def drain_rows(k, carry):
        for copy in in_copies(k):
            copy.wait_recv()
        return carry

    lax.fori_loop(0, NCHUNK, drain_rows, 0)
    per_core(drain_gather)
    for exchange in (*masks, *lses, stats, dns, dhs, gvs, gys, gzs):
        exchange.drain()


def solution(mesh):
    def local_step(hidden, norm_gain, emb_table, labels, tok_mask):
        rows, seq_len, width = hidden.shape
        any_space = pl.BlockSpec(memory_space=pl.ANY)
        vmem = pl.BlockSpec(memory_space=pltpu.VMEM)
        smem = pl.BlockSpec(memory_space=pltpu.SMEM)
        v, sem = pltpu.VMEM, pltpu.SemaphoreType.DMA
        row8, wide8, block_f32 = v((8, TOK), F32), v((8, NALL), F32), v((TOK, WIDTH), F32)
        table, _, d_hidden, d_gain, loss = pl.pallas_call(
            step_kernel,
            in_specs=[vmem, vmem, vmem, vmem, any_space],
            out_specs=[any_space, any_space, vmem, vmem, smem],
            out_shape=[
                jax.ShapeDtypeStruct((VLOC, WIDTH), F32),
                jax.ShapeDtypeStruct((NZ, NY, TOK, WIDTH), F32),
                jax.ShapeDtypeStruct((TOK, WIDTH), BF16),
                jax.ShapeDtypeStruct((WIDTH,), F32),
                jax.ShapeDtypeStruct((1, 1), F32),
            ],
            scratch_shapes=[
                block_f32, v((TOK, WIDTH), BF16), v((NV, 8, TOK), F32), v((2, VT, WIDTH), BF16), v((VTAIL, WIDTH), BF16),
                row8, row8, row8, wide8, row8, wide8, wide8, wide8,
                v((NALL, WIDTH), BF16), v((TILE, WIDTH), F32), v((2, PAIR, WIDTH), BF16), v((SLOTS, PAIR, WIDTH), F32),
                v((NZ, PAIR, WIDTH), F32), block_f32, v((NV, SLICE, WIDTH), F32), block_f32,
                v((NV, 8, WIDTH), F32), v((NY, 8, WIDTH), F32), v((NZ, 8, WIDTH), F32),
                sem((3,)), sem((2,)), sem((2 * NMSG,)), sem((NMSG,)), sem((NMSG,)), sem((NZ,)), sem((2, 2)),
                sem((SLOTS, 2)), sem((SLOTS, 8)), sem((NCHUNK, 8)),
                sem((2, 7)), sem((2, 3)), sem((2, 7)), sem((2, 3)), sem((2, 7)),
                sem((2, 7)), sem((2, 7)), sem((2, 7)), sem((2, 3)), sem((2, 7)),
            ],
            compiler_params=pltpu.CompilerParams(
                collective_id=0, has_side_effects=True, vmem_limit_bytes=63 * 2**20 + 2**19
            ),
            name="head_step",
        )(hidden.reshape(rows * seq_len, width), norm_gain, labels, tok_mask, emb_table)
        return loss[0, 0], table, d_hidden.reshape(rows, seq_len, width), d_gain

    return jax.shard_map(
        local_step,
        mesh=mesh,
        in_specs=(P("dp", None, None), P(None), P("vp", None), P("dp", None), P("dp", None)),
        out_specs=(P(), P("vp", None), P("dp", None, None), P(None)),
        check_vma=False,
    )
```
